32 devices in a mesh: hx: 4 (over y, x), hy: 4 (over z), tok: 2 (over core).
Axes of the slice: x: 2, y: 2, z: 4, core: 2. Of those that a mesh axis runs over, the one named last changes fastest.
Arguments:
- stream_in: bfloat16 [512, 4608], P('tok', ('hx', 'hy')), may hold values from -6 to 6
- before_gain: bfloat16 [4608], P(('hx', 'hy')), may hold values from 0.25 to 1.75
- after_gain: bfloat16 [4608], P(('hx', 'hy')), may hold values from 0.25 to 1.75
- feed_gain: bfloat16 [4608], P(('hx', 'hy')), may hold values from 0.25 to 1.75
- query_weight: bfloat16 [4608, 4096], P('tok', ('hx', 'hy')), may hold values from -1 to 1
- key_weight: bfloat16 [4608, 2048], P('tok', ('hx', 'hy')), may hold values from -64 to 64
- value_weight: bfloat16 [4608, 2048], P('tok', ('hx', 'hy')), may hold values from -0.09375 to 0.09375
- output_weight: bfloat16 [4096, 4608], P(('hx', 'hy'), 'tok'), may hold values from -0.09375 to 0.09375
- documents: int32 [512], P('tok'), may hold values from 0 to 7, never falling along the last dimension, each value on 1 to 128 neighbouring positions
Outputs:
- residual: bfloat16 [512, 4608], P('tok', ('hx', 'hy'))
- feed_input: bfloat16 [512, 4608], P('tok', ('hx', 'hy'))
The draws below stay inside these ranges and needn't reach their ends.
Inputs may be any that keep to these rules, and one draw needn't show every extreme that they name: `documents`: ids never fall along the tokens; a document holds at most 128 tokens and may run across a sequence's end.
All inputs are finite; a program needn't handle non-finite values.
Results may differ from the reference program's by a relative error of at most 0.014.
The reference program's roundings to bfloat16 on the way count: a program that leaves them out, or rounds other values in their place, can miss the bound.
Values may be sent and summed in bfloat16 or wider, within the bound.
A program may use at most 64 MiB of HBM per device.

```python
import math
import jax
import jax.numpy as jnp
import numpy as np
from jax import lax

D = 4608
QH = 32
KVH = 16
HEAD = 128
LENGTH = 256
TOKENS = 512
DOCS = 8
N_HX = 4
N_HY = 4


def query_base(key):
    return jax.random.truncated_normal(jax.random.fold_in(key, 11), -6.0, 6.0, (D, QH * HEAD), jnp.float32) * D ** (-0.5)


def draw_query_weight(key, part):
    return query_base(key).astype(jnp.bfloat16)


def draw_key_weight(key, part):
    independent = jax.random.truncated_normal(jax.random.fold_in(key, 23), -6.0, 6.0, (D, KVH * HEAD), jnp.float32) * D ** (-0.5)
    return independent.astype(jnp.bfloat16)


def steps_of(stream_key, shape, split, smallest, high):
    def one(position, shards_of):
        heights = jax.random.uniform(jax.random.fold_in(jax.random.fold_in(stream_key, 6), position), (shards_of,), jnp.float32, smallest / len(split), high / len(split))
        return jnp.repeat(jnp.exp(heights), shape[position] // shards_of).reshape((-1,) + (1,) * (len(shape) - position - 1))

    level = one(*split[0])
    for cut in split[1:]:
        level = level * one(*cut)
    return level


def split_up(amount, total, bound, lean):
    weights = [(1 << 20) // math.isqrt(standing ** lean) + 1 for standing in range(2, amount + 1)]
    surplus, counts = total - bound - (amount - 1), [1] * (amount - 1)
    while surplus > 0:
        candidates = [i for i in range(amount - 1) if counts[i] < bound]
        whole, left = sum([weights[i] for i in candidates]), surplus
        for i in candidates:
            more = min(bound - counts[i], max(1, left * weights[i] // whole), surplus)
            counts[i] = counts[i] + more
            surplus = surplus - more
    return np.array([bound] + counts)


def uneven_parts(rng, amount, total, limit, skew):
    if amount == 2:
        one = jax.random.randint(rng, (), max(1, total - limit), min(limit, total - 1) + 1)
        return jnp.stack([one, total - one])
    lengths = jnp.asarray(split_up(amount, total, limit, skew), jnp.int32)
    pairs = (amount - 1) // 2
    donor, receiver = lengths[1:1 + 2 * pairs:2], lengths[2:2 + 2 * pairs:2]
    margin = jnp.minimum(donor - 1, limit - receiver)
    passed = jax.random.randint(jax.random.fold_in(rng, 1), (pairs,), 0, 1 << 20) % (margin + 1)
    lengths = lengths.at[1:1 + 2 * pairs:2].set(donor - passed).at[2:2 + 2 * pairs:2].set(receiver + passed)
    return lengths[jax.random.permutation(jax.random.fold_in(rng, 2), amount)]


def scatter_about(stream_key, shape, width, reach, cuts=(), kind=jnp.bfloat16):
    values = jax.random.normal(stream_key, shape, jnp.float32) * width
    if len(cuts) > 0:
        values = steps_of(stream_key, shape, cuts, -0.22, 0.18) * values
    return jnp.clip(values, min=-reach, max=reach).astype(kind)


def setup_inputs(seed: int = 0) -> dict:
    seeds = jax.random.split(jax.random.key(seed), 10)
    stream_in = scatter_about(seeds[0], (TOKENS, D), 1.0, 6.0, ((0, 2), (1, 16)))
    before_gain = jnp.clip(1.0 + 0.15 * jax.random.normal(seeds[1], (D,), jnp.float32), 0.25, 1.75).astype(jnp.bfloat16)
    after_gain = jnp.clip(1.0 + 0.15 * jax.random.normal(seeds[2], (D,), jnp.float32), 0.25, 1.75).astype(jnp.bfloat16)
    feed_gain = jnp.clip(1.0 + 0.15 * jax.random.normal(seeds[3], (D,), jnp.float32), 0.25, 1.75).astype(jnp.bfloat16)
    query_weight = draw_query_weight(jax.random.fold_in(seeds[9], 71), 0)
    key_weight = draw_key_weight(jax.random.fold_in(seeds[9], 71), 0)
    value_weight = scatter_about(seeds[6], (D, KVH * HEAD), D ** -0.5, 0.09375, ((0, 2), (1, 16)))
    output_weight = scatter_about(seeds[7], (QH * HEAD, D), (QH * HEAD) ** -0.5, 0.09375, ((0, 16), (1, 2)))
    documents = jnp.searchsorted(jnp.cumsum(uneven_parts(seeds[8], DOCS, TOKENS, LENGTH // 2, 0)), jnp.arange(TOKENS), side="right").astype(jnp.int32)
    return {"stream_in": stream_in, "before_gain": before_gain, "after_gain": after_gain, "feed_gain": feed_gain, "query_weight": query_weight, "key_weight": key_weight, "value_weight": value_weight, "output_weight": output_weight, "documents": documents}


epsilon = 1e-06
neg_big = -1e+30

def rotate(values, positions):
    half_width = values.shape[-1] // 2
    frequency = 10000.0 ** (-jnp.arange(half_width, dtype=jnp.float32) / half_width)
    angles = positions.astype(jnp.float32)[:, None] * frequency[None, :]
    cosine_table = jnp.cos(angles)[:, None, :]
    sine_table = jnp.sin(angles)[:, None, :]
    leading = values[..., :half_width]
    trailing = values[..., half_width:]
    return jnp.concatenate([leading * cosine_table - trailing * sine_table, trailing * cosine_table + leading * sine_table], axis=-1)

def norm_rows(values, gain):
    squares = lax.optimization_barrier(jnp.sum(values * values, axis=-1, keepdims=True))
    return values * lax.rsqrt(squares / D + epsilon) * gain.astype(jnp.float32)[None, :]

def reference(stream_in, before_gain, after_gain, feed_gain, query_weight, key_weight, value_weight, output_weight, documents):
    wide = stream_in.astype(jnp.float32)
    normed = norm_rows(wide, before_gain).astype(jnp.bfloat16)
    positions = (jnp.arange(TOKENS) % LENGTH).astype(jnp.int32)
    query_sum = jnp.dot(normed, query_weight, preferred_element_type=jnp.float32)
    key_sum = jnp.dot(normed, key_weight, preferred_element_type=jnp.float32)
    value_sum = jnp.dot(normed, value_weight, preferred_element_type=jnp.float32)
    queries = (rotate(query_sum.reshape(TOKENS, QH, HEAD), positions) * (D / QH) ** (-0.5)).astype(jnp.bfloat16)
    keys = rotate(key_sum.reshape(TOKENS, KVH, HEAD), positions).astype(jnp.bfloat16)
    values = value_sum.reshape(TOKENS, KVH, HEAD).astype(jnp.bfloat16)
    ratio = QH // KVH
    count_seq = TOKENS // LENGTH
    query_seq = queries.reshape(count_seq, LENGTH, KVH, ratio, HEAD)
    key_seq = keys.reshape(count_seq, LENGTH, KVH, HEAD)
    value_seq = values.reshape(count_seq, LENGTH, KVH, HEAD)
    doc_seq = documents.reshape(count_seq, LENGTH)

    def one_sequence(items):
        query_part, key_part, value_part, doc_part = items
        scores = jnp.einsum('tkrh,skh->tkrs', query_part.astype(jnp.float32), key_part.astype(jnp.float32))
        index = jnp.arange(LENGTH)
        allowed = (index[None, :] <= index[:, None]) & (doc_part[None, :] == doc_part[:, None])
        mask = allowed[:, None, None, :]
        best = lax.optimization_barrier(jnp.max(jnp.where(mask, scores, neg_big), axis=-1, keepdims=True))
        weights = jnp.where(mask, jnp.exp(scores - best), 0.0)
        total = lax.optimization_barrier(jnp.sum(weights, axis=-1))
        weights_low = lax.optimization_barrier(weights.astype(jnp.bfloat16)).astype(jnp.float32)
        summed = jnp.einsum('tkrs,skh->tkrh', weights_low, value_part.astype(jnp.float32))
        return (summed / total[..., None]).astype(jnp.bfloat16)
    attended = lax.map(one_sequence, (query_seq, key_seq, value_seq, doc_seq)).reshape(TOKENS, QH * HEAD)
    groups = N_HX * N_HY
    span = QH * HEAD // groups
    mixed = jnp.zeros((TOKENS, D), jnp.float32)
    for group in range(groups):
        term = jnp.dot(attended[:, group * span:(group + 1) * span], output_weight[group * span:(group + 1) * span, :], preferred_element_type=jnp.float32)
        mixed = mixed + lax.optimization_barrier(term.astype(jnp.bfloat16)).astype(jnp.float32)
    residual = (wide + norm_rows(mixed, after_gain)).astype(jnp.bfloat16)
    feed_input = norm_rows(residual.astype(jnp.float32), feed_gain).astype(jnp.bfloat16)
    return (residual, feed_input)
```

```python
import functools

import jax
import jax.numpy as jnp
import numpy as np
from jax import lax
from jax.experimental import pallas as pl
from jax.experimental.pallas import tpu as pltpu
from jax.sharding import PartitionSpec as P

D = 4608
QH = 32
HEAD = 128
LENGTH = 256
LANES = 128

epsilon = 1e-06
neg_big = -1e30
MESH = pl.DeviceIdType.MESH
F32 = jnp.float32
BF16 = jnp.bfloat16


def flip(index, mask):
    low = (index % 2 + mask % 2) % 2
    high = (index // 2 + mask // 2) % 2
    return low + 2 * high


def rope_tables():
    half = HEAD // 2
    frequency = (10000.0 ** (-np.arange(half, dtype=np.float32) / half)).astype(np.float32)
    angles = np.arange(LENGTH, dtype=np.float32)[:, None] * frequency[None, :]
    cosine, sine = np.cos(angles), np.sin(angles)
    table = np.stack([np.concatenate([cosine, cosine], 1), np.concatenate([-sine, sine], 1)])
    return table.astype(np.float32)


def kernel(
    paired,
    stream, gains, docs, tables, wq, wk, wv, wo,
    residual_out, feed_out,
    raw, slots, docs_v, tables_v, weights, out_weight, out_main, out_tail,
    terms, first_a, first_b, from_x, from_y, from_z, stats, stats_in, stats_mid, stats_zin,
    local_sem, weight_send, weight_recv, gather_send, gather_recv, reduce_send, reduce_recv,
    stat_send, stat_recv,
):
    rows, width = raw.shape
    full, rest = width // LANES, width % LANES
    per = LANES // rest
    tail_rows = rows // per
    body = full * rows
    size = body + tail_rows
    a, b, c = lax.axis_index("hx"), lax.axis_index("hy"), lax.axis_index("tok")
    along_x, along_y, across = flip(a, 1), flip(a, 2), flip(a, 3)
    z_peers = [None] + [flip(b, j) for j in (1, 2, 3)]

    def group_of(i, j):
        return flip(a, i) * 4 + flip(b, j)

    locals_ = [
        pltpu.make_async_copy(stream, raw, local_sem.at[0]),
        pltpu.make_async_copy(gains, slots.at[0, pl.ds(size, 16)], local_sem.at[1]),
        pltpu.make_async_copy(docs, docs_v, local_sem.at[2]),
        pltpu.make_async_copy(tables, tables_v, local_sem.at[3]),
    ]
    for copy in locals_:
        copy.start()
    wrows, qcols, kcols = wq.shape[0], wq.shape[1], wk.shape[1]
    shard = c if paired else 0
    start = pl.multiple_of(shard * wrows, 16)
    targets = [
        (wo, out_weight.at[shard]),
        (wq, weights.at[pl.ds(start, wrows), pl.ds(0, qcols)]),
        (wk, weights.at[pl.ds(start, wrows), pl.ds(qcols, kcols)]),
        (wv, weights.at[pl.ds(start, wrows), pl.ds(qcols + kcols, kcols)]),
    ]
    weight_local = [
        pltpu.make_async_copy(src, dst, local_sem.at[4 + k]) for k, (src, dst) in enumerate(targets)
    ]

    barrier = pltpu.get_barrier_semaphore()
    greet = [{"hx": along_x}, {"hx": along_y}, {"hx": across}]
    greet += [{"hy": z_peers[j]} for j in (1, 2, 3)]
    if paired:
        greet.append({"tok": 1 - c})
    for peer in greet:
        pl.semaphore_signal(barrier, inc=1, device_id=peer, device_id_type=MESH)
    for copy in weight_local:
        copy.start()

    lane = lax.broadcasted_iota(jnp.int32, (tail_rows, LANES), 1)
    locals_[0].wait()
    for k in range(full):
        slots[0, k * rows:(k + 1) * rows, :] = raw[:, k * LANES:(k + 1) * LANES]
    tail = raw[:, full * LANES:width].astype(F32)
    packed = jnp.concatenate(
        [tail[r * tail_rows:(r + 1) * tail_rows] for r in range(per)], axis=1
    )
    slots[0, body:size, :] = packed.astype(BF16)
    locals_[1].wait()
    pl.semaphore_wait(barrier, len(greet))

    def remote(src, dst, send, recv, peer):
        return pltpu.make_async_remote_copy(
            src_ref=src, dst_ref=dst, send_sem=send, recv_sem=recv, device_id=peer, device_id_type=MESH
        )

    total_rows = size + 16
    cut = (total_rows // 32) * 16

    def gather_z(j):
        return remote(slots.at[0], slots.at[j], gather_send.at[j], gather_recv.at[j], {"hy": z_peers[j]})

    def gather_x(j):
        return remote(slots.at[j], slots.at[4 + j], gather_send.at[4 + j], gather_recv.at[4 + j], {"hx": along_x})

    def gather_y(j):
        return remote(slots.at[j], slots.at[8 + j], gather_send.at[8 + j], gather_recv.at[8 + j], {"hx": along_y})

    def relay_a(j):
        part = pl.ds(0, cut)
        return remote(
            slots.at[4 + j, part], slots.at[12 + j, part], gather_send.at[12 + j], gather_recv.at[12 + j], {"hx": along_y}
        )

    def relay_b(j):
        part = pl.ds(cut, total_rows - cut)
        return remote(
            slots.at[8 + j, part], slots.at[12 + j, part], gather_send.at[16 + j], gather_recv.at[16 + j], {"hx": along_x}
        )

    gather_x(0).start()
    gather_y(0).start()
    for j in (1, 2, 3):
        gather_z(j).start()
    weight_remote = []
    if paired:
        weight_remote = [
            remote(src, dst, weight_send.at[k], weight_recv.at[k], {"tok": 1 - c})
            for k, (src, dst) in enumerate(targets)
        ]
        for copy in weight_remote:
            copy.start()

    def forward(j):
        gather_z(j).wait_recv()
        gather_x(j).start()
        gather_y(j).start()

    def relay(j):
        gather_x(j).wait_recv()
        relay_a(j).start()
        gather_y(j).wait_recv()
        relay_b(j).start()

    shards = out_weight.shape[0]
    per_shard = 16 // shards

    def prepare_out(g):
        offset = (g % per_shard) * width
        base = offset // LANES * LANES
        shift = offset - base
        span = (full + 1) * LANES
        piece = out_weight[g // per_shard, :, base:base + span].astype(F32)
        if shift:
            piece = pltpu.roll(piece, span - shift, 1)
        piece = piece.astype(BF16)
        out_main[g] = piece[:, :full * LANES]
        return piece[:, full * LANES:].astype(F32)

    def prepare_outs(q):
        wide_lane = lax.broadcasted_iota(jnp.int32, (out_weight.shape[1], LANES), 1)
        held = None
        for r in range(per):
            part = prepare_out(q * per + r)
            if r:
                part = pltpu.roll(part, r * rest, 1)
            held = part if r == 0 else jnp.where(wide_lane // rest == r, part, held)
        out_tail[:, q * LANES:(q + 1) * LANES] = held.astype(BF16)

    forward(1)
    relay(0)
    weight_local[0].wait()
    if paired:
        weight_remote[0].wait_recv()
    prepare_outs(0)
    forward(2)
    relay(1)
    prepare_outs(1)
    forward(3)
    relay(2)
    prepare_outs(2)
    prepare_outs(3)
    locals_[2].wait()
    locals_[3].wait()
    doc_col = jnp.concatenate([docs_v[...]] * (LANES // 8), axis=0).T[:, 0:1]
    doc_row = docs_v[0:1, :]
    t_index = lax.broadcasted_iota(jnp.int32, (LENGTH, LENGTH), 0)
    s_index = lax.broadcasted_iota(jnp.int32, (LENGTH, LENGTH), 1)
    for copy in weight_local[1:]:
        copy.wait()
    if paired:
        for copy in weight_remote[1:]:
            copy.wait_recv()
    relay(3)
    for j in range(4):
        relay_a(j).wait_recv()
        relay_b(j).wait_recv()

    def tails_of(i):
        out = []
        for r in range(per):
            held = None
            for j in range(per):
                part = slots[4 * i + j, body:size, :].astype(F32)
                move = (rest * (j - r)) % LANES
                if move:
                    part = pltpu.roll(part, move, 1)
                held = part if j == 0 else jnp.where(lane // rest == j, part, held)
            out.append(held)
        return jnp.concatenate(out, axis=0)

    squares = jnp.zeros((rows, LANES), F32)
    tails = []
    for i in range(4):
        for j in range(4):
            for k in range(full):
                part = slots[4 * i + j, k * rows:(k + 1) * rows, :].astype(F32)
                squares = squares + part * part
        unpacked = tails_of(i)
        tails.append(unpacked)
        squares = squares + unpacked * unpacked
    first_sq = jnp.sum(squares, axis=1, keepdims=True)
    first_scale = lax.rsqrt(first_sq / D + epsilon)
    sums = None
    lane_row = lax.broadcasted_iota(jnp.int32, (1, LANES), 1)
    for i in range(4):
        columns, w_main, w_tail = [], [], []
        tail_gain = None
        for j in range(4):
            gain = slots[4 * i + j, size:size + 16, :].astype(F32)
            for k in range(full):
                part = slots[4 * i + j, k * rows:(k + 1) * rows, :].astype(F32)
                columns.append((part * first_scale * gain[k:k + 1]).astype(BF16))
            last = gain[full:full + 1]
            tail_gain = last if j == 0 else jnp.where(lane_row // rest == j, last, tail_gain)
            at = group_of(i, j) * width
            w_main.append(weights[pl.ds(pl.multiple_of(at, 16), full * LANES), :])
            w_tail.append(weights[pl.ds(pl.multiple_of(at + full * LANES, 16), rest), :])
        columns.append((tails[i] * first_scale * tail_gain).astype(BF16))
        part = jnp.dot(
            jnp.concatenate(columns, axis=1), jnp.concatenate(w_main + w_tail, axis=0), preferred_element_type=F32
        )
        sums = part if sums is None else sums + part

    cosine, sine = tables_v[0], tables_v[1]

    def rope(x):
        return x * cosine + pltpu.roll(x, HEAD // 2, 1) * sine

    query_heads, key_heads = qcols // HEAD, kcols // HEAD
    ratio = query_heads // key_heads
    allowed = (s_index <= t_index) & (doc_row == doc_col)
    attended = []
    for h in range(query_heads):
        kv = h // ratio
        query = (rope(sums[:, h * HEAD:(h + 1) * HEAD]) * (D / QH) ** (-0.5)).astype(BF16)
        key = rope(sums[:, qcols + kv * HEAD:qcols + (kv + 1) * HEAD]).astype(BF16)
        value = sums[:, qcols + kcols + kv * HEAD:qcols + kcols + (kv + 1) * HEAD].astype(BF16)
        scores = lax.dot_general(query, key, (((1,), (1,)), ((), ())), preferred_element_type=F32)
        best = jnp.max(jnp.where(allowed, scores, neg_big), axis=1, keepdims=True)
        soft = jnp.where(allowed, jnp.exp(scores - best), 0.0)
        total = jnp.sum(soft, axis=1, keepdims=True)
        mixed_values = jnp.dot(soft.astype(BF16), value, preferred_element_type=F32)
        attended.append((mixed_values / total).astype(BF16))
    attended = jnp.concatenate(attended, axis=1)

    for q in range(4):
        tail_terms = jnp.dot(attended, out_tail[:, q * LANES:(q + 1) * LANES], preferred_element_type=F32)
        for r in range(per):
            g = q * per + r
            main = jnp.dot(attended, out_main[g], preferred_element_type=F32).astype(BF16)
            for k in range(full):
                terms[g, k * rows:(k + 1) * rows, :] = main[:, k * LANES:(k + 1) * LANES]
            held = None
            for s in range(per):
                part = tail_terms[s * tail_rows:(s + 1) * tail_rows]
                move = (rest * (s - r)) % LANES
                if move:
                    part = pltpu.roll(part, move, 1)
                held = part if s == 0 else jnp.where(lane // rest == s, part, held)
            terms[g, body:size, :] = held.astype(BF16)

    half = size // 2
    top, bottom = pl.ds(0, half), pl.ds(half, half)

    def diagonal_a(j):
        return remote(
            terms.at[group_of(3, j), top], first_a.at[j], reduce_send.at[j], reduce_recv.at[j], {"hx": along_x}
        )

    def diagonal_b(j):
        return remote(
            terms.at[group_of(3, j), bottom], first_b.at[j], reduce_send.at[4 + j], reduce_recv.at[4 + j], {"hx": along_y}
        )

    def reduce_x(j):
        return remote(
            terms.at[group_of(1, j)], from_x.at[j], reduce_send.at[8 + j], reduce_recv.at[8 + j], {"hx": along_x}
        )

    def reduce_y(j):
        return remote(
            terms.at[group_of(2, j)], from_y.at[j], reduce_send.at[12 + j], reduce_recv.at[12 + j], {"hx": along_y}
        )

    def reduce_z(j):
        return remote(
            terms.at[group_of(0, j)], from_z.at[j - 1], reduce_send.at[15 + j], reduce_recv.at[15 + j], {"hy": z_peers[j]}
        )

    order = (3, 2, 1, 0)
    for j in order:
        diagonal_a(j).start()
        diagonal_b(j).start()

    def second(j):
        diagonal_a(j).wait_recv()
        g = group_of(2, j)
        terms[g, top, :] = (terms[g, top, :].astype(F32) + first_a[j].astype(F32)).astype(BF16)
        reduce_y(j).start()
        diagonal_b(j).wait_recv()
        g = group_of(1, j)
        terms[g, bottom, :] = (terms[g, bottom, :].astype(F32) + first_b[j].astype(F32)).astype(BF16)
        reduce_x(j).start()

    def plane_sum(j):
        reduce_x(j).wait_recv()
        reduce_y(j).wait_recv()
        return terms[group_of(0, j)].astype(F32) + from_x[j].astype(F32) + from_y[j].astype(F32)

    for j in order:
        second(j)
    for j in (3, 2, 1):
        terms[group_of(0, j)] = plane_sum(j).astype(BF16)
        reduce_z(j).start()
    mixed = plane_sum(0)
    for j in (3, 2, 1):
        reduce_z(j).wait_recv()
        mixed = mixed + from_z[j - 1].astype(F32)

    gain = slots[0, size:size + 16, :].astype(F32)
    pieces = [mixed[k * rows:(k + 1) * rows] for k in range(full)]
    last = []
    for r in range(per):
        part = mixed[body:size]
        if r:
            part = pltpu.roll(part, LANES - r * rest, 1)
        last.append(jnp.where(lane < rest, part, 0.0))
    pieces.append(jnp.concatenate(last, axis=0))
    wides = [raw[:, k * LANES:(k + 1) * LANES].astype(F32) for k in range(full)]
    own = tails[0]
    padded = jnp.concatenate([raw[:, full * LANES:width].astype(F32), jnp.zeros((rows, LANES - rest), F32)], axis=1)
    wides.append(padded)
    squares = cross = branch_sq = jnp.zeros((rows, LANES), F32)
    for k in range(full + 1):
        branch = pieces[k] * gain[full + 1 + k:full + 2 + k]
        squares = squares + pieces[k] * pieces[k]
        cross = cross + wides[k] * branch
        branch_sq = branch_sq + branch * branch
    all_lane = lax.broadcasted_iota(jnp.int32, (rows, LANES), 1)
    three = jnp.where(
        all_lane == 0,
        jnp.sum(squares, axis=1, keepdims=True),
        jnp.where(
            all_lane == 1,
            jnp.sum(cross, axis=1, keepdims=True),
            jnp.sum(branch_sq, axis=1, keepdims=True),
        ),
    )
    stats[...] = three.T[0:8]
    plane = (None, along_x, along_y, across)

    def stat_plane(i):
        return remote(stats, stats_in.at[i - 1], stat_send.at[i - 1], stat_recv.at[i - 1], {"hx": plane[i]})

    def stat_z(j):
        return remote(stats_mid, stats_zin.at[j - 1], stat_send.at[2 + j], stat_recv.at[2 + j], {"hy": z_peers[j]})

    for i in (3, 2, 1):
        stat_plane(i).start()
    for i in (1, 2, 3):
        stat_plane(i).wait_recv()
    stats_mid[...] = stats[...] + stats_in[0] + stats_in[1] + stats_in[2]
    for j in (3, 2, 1):
        stat_z(j).start()
    for j in (1, 2, 3):
        stat_z(j).wait_recv()
    summed = stats_mid[...] + stats_zin[0] + stats_zin[1] + stats_zin[2]
    back = jnp.concatenate([summed] * (LANES // 8), axis=0).T
    after_sq, cross_sum, branch_sum = back[:, 0:1], back[:, 1:2], back[:, 2:3]
    after_scale = lax.rsqrt(after_sq / D + epsilon)
    feed_sq = first_sq + 2.0 * after_scale * cross_sum + after_scale * after_scale * branch_sum
    feed_scale = lax.rsqrt(feed_sq / D + epsilon)
    for k in range(full + 1):
        n = LANES if k < full else rest
        residual = (wides[k] + pieces[k] * after_scale * gain[full + 1 + k:full + 2 + k]).astype(BF16)
        feed = (residual.astype(F32) * feed_scale * gain[2 * full + 2 + k:2 * full + 3 + k]).astype(BF16)
        residual_out[:, k * LANES:k * LANES + n] = residual[:, :n]
        feed_out[:, k * LANES:k * LANES + n] = feed[:, :n]

    for j in range(4):
        gather_x(j).wait_send()
        gather_y(j).wait_send()
        relay_a(j).wait_send()
        relay_b(j).wait_send()
        diagonal_a(j).wait_send()
        diagonal_b(j).wait_send()
        reduce_x(j).wait_send()
        reduce_y(j).wait_send()
    for j in (1, 2, 3):
        gather_z(j).wait_send()
        reduce_z(j).wait_send()
        stat_plane(j).wait_send()
        stat_z(j).wait_send()
    for copy in weight_remote:
        copy.wait_send()


def per_device(paired, stream_in, before_gain, after_gain, feed_gain, query_weight, key_weight, value_weight, output_weight, documents):
    rows, width = stream_in.shape
    full, rest = width // LANES, width % LANES
    per = LANES // rest
    size = full * rows + rows // per
    if not paired:
        query_weight, key_weight, value_weight = (
            lax.all_gather(piece, "tok", axis=0, tiled=True) for piece in (query_weight, key_weight, value_weight)
        )
        output_weight = lax.all_gather(output_weight, "tok", axis=1, tiled=True)

    def laid(gain):
        return jnp.concatenate([gain[:full * LANES], jnp.tile(gain[full * LANES:], per)])

    gains = jnp.concatenate([laid(before_gain), laid(after_gain), laid(feed_gain)]).reshape(-1, LANES)
    gains = jnp.pad(gains, ((0, 16 - gains.shape[0]), (0, 0)))
    docs = jnp.broadcast_to(documents.astype(F32)[None], (8, rows))
    tables = jnp.asarray(rope_tables())
    qcols, kcols = query_weight.shape[1], key_weight.shape[1]
    shards = 2 if paired else 1
    depth = output_weight.shape[0]
    any_spec = pl.BlockSpec(memory_space=pl.ANY)
    vmem = pl.BlockSpec(memory_space=pltpu.VMEM)
    dma = pltpu.SemaphoreType.DMA
    return pl.pallas_call(
        functools.partial(kernel, paired),
        out_shape=[jax.ShapeDtypeStruct((rows, width), BF16)] * 2,
        in_specs=[any_spec] * 8,
        out_specs=[vmem] * 2,
        scratch_shapes=[
            pltpu.VMEM((rows, width), BF16),
            pltpu.VMEM((16, size + 16, LANES), BF16),
            pltpu.VMEM((8, rows), F32),
            pltpu.VMEM((2, LENGTH, HEAD), F32),
            pltpu.VMEM((D, qcols + 2 * kcols), BF16),
            pltpu.VMEM((shards, depth, output_weight.shape[1]), BF16),
            pltpu.VMEM((16, depth, full * LANES), BF16),
            pltpu.VMEM((depth, 4 * LANES), BF16),
            pltpu.VMEM((16, size, LANES), BF16),
            pltpu.VMEM((4, size // 2, LANES), BF16),
            pltpu.VMEM((4, size // 2, LANES), BF16),
            pltpu.VMEM((4, size, LANES), BF16),
            pltpu.VMEM((4, size, LANES), BF16),
            pltpu.VMEM((3, size, LANES), BF16),
            pltpu.VMEM((8, rows), F32),
            pltpu.VMEM((3, 8, rows), F32),
            pltpu.VMEM((8, rows), F32),
            pltpu.VMEM((3, 8, rows), F32),
            dma((8,)),
            dma((4,)),
            dma((4,)),
            dma((20,)),
            dma((20,)),
            dma((19,)),
            dma((19,)),
            dma((6,)),
            dma((6,)),
        ],
        compiler_params=pltpu.CompilerParams(
            collective_id=0, has_side_effects=True, vmem_limit_bytes=56 * 1024 * 1024
        ),
    )(stream_in, gains, docs, tables, query_weight, key_weight, value_weight, output_weight)


def solution(mesh):
    both = ("hx", "hy")
    in_specs = (
        P("tok", both),
        P(both),
        P(both),
        P(both),
        P("tok", both),
        P("tok", both),
        P("tok", both),
        P(both, "tok"),
        P("tok"),
    )
    out_specs = (P("tok", both), P("tok", both))
    paired = mesh.shape["tok"] == 2
    return jax.shard_map(
        functools.partial(per_device, paired), mesh=mesh, in_specs=in_specs, out_specs=out_specs, check_vma=False
    )
```

```python
import functools

import jax
import jax.numpy as jnp
import numpy as np
from jax import lax
from jax.experimental import pallas as pl
from jax.experimental.pallas import tpu as pltpu
from jax.sharding import PartitionSpec as P

D = 4608
QH = 32
HEAD = 128
LENGTH = 256
LANES = 128

epsilon = 1e-06
neg_big = -1e30
MESH = pl.DeviceIdType.MESH
F32 = jnp.float32
BF16 = jnp.bfloat16


def flip(index, mask):
    low = (index % 2 + mask % 2) % 2
    high = (index // 2 + mask // 2) % 2
    return low + 2 * high


def rope_tables():
    half = HEAD // 2
    frequency = (10000.0 ** (-np.arange(half, dtype=np.float32) / half)).astype(np.float32)
    angles = frequency[:, None] * np.arange(LENGTH, dtype=np.float32)[None, :]
    return np.stack([np.cos(angles), np.sin(angles)]).astype(np.float32)


def tall_row(row):
    return jnp.broadcast_to(row, (8, row.shape[1]))


def tall(block):
    return jnp.concatenate([block] * (LANES // block.shape[0]), axis=0).T


def kernel(
    paired,
    stream, small, tables, wq, wk, wv, wo,
    residual_out, feed_out,
    slots, small_v, tables_v, weights, out_weight, out_t, acc,
    terms, first_a, first_b, from_x, from_y, from_z,
    head, head_z, head_mid, head_plane, stats, stats_in, stats_mid, stats_zin,
    local_sem, weight_send, weight_recv, gather_send, gather_recv, reduce_send, reduce_recv,
    head_send, head_recv, stat_send, stat_recv,
):
    width, rows = stream.shape
    rest = width - rows
    a, b, c = lax.axis_index("hx"), lax.axis_index("hy"), lax.axis_index("tok")
    along_x, along_y, across = flip(a, 1), flip(a, 2), flip(a, 3)
    plane = (None, along_x, along_y, across)
    z_peers = [None] + [flip(b, j) for j in (1, 2, 3)]

    def offset_of(i, j):
        return pl.multiple_of((flip(a, i) * 4 + flip(b, j)) * width, 16)

    locals_ = [
        pltpu.make_async_copy(stream, slots.at[0], local_sem.at[0]),
        pltpu.make_async_copy(small, small_v, local_sem.at[1]),
        pltpu.make_async_copy(tables, tables_v, local_sem.at[2]),
    ]
    for copy in locals_:
        copy.start()
    wrows, qcols, kcols = wq.shape[0], wq.shape[1], wk.shape[1]
    shard = c if paired else 0
    start = pl.multiple_of(shard * wrows, 16)
    targets = [
        (wq, weights.at[pl.ds(start, wrows), pl.ds(0, qcols)]),
        (wk, weights.at[pl.ds(start, wrows), pl.ds(qcols, kcols)]),
        (wv, weights.at[pl.ds(start, wrows), pl.ds(qcols + kcols, kcols)]),
        (wo, out_weight.at[shard]),
    ]
    weight_local = [
        pltpu.make_async_copy(src, dst, local_sem.at[3 + k]) for k, (src, dst) in enumerate(targets)
    ]

    barrier = pltpu.get_barrier_semaphore()
    greet = [{"hx": along_x}, {"hx": along_y}, {"hx": across}]
    greet += [{"hy": z_peers[j]} for j in (1, 2, 3)]
    if paired:
        greet.append({"tok": 1 - c})
    for peer in greet:
        pl.semaphore_signal(barrier, inc=1, device_id=peer, device_id_type=MESH)
    for copy in weight_local:
        copy.start()

    row8 = lax.broadcasted_iota(jnp.int32, (8, rows), 0)
    locals_[0].wait()
    locals_[1].wait()
    own = slots[0].astype(F32)
    small_rows = small_v[...]
    padded_tail = jnp.concatenate([small_rows[1:2, rows:rows + LANES], jnp.zeros((1, rows - LANES), F32)], axis=1)
    head[...] = jnp.where(
        row8 == 0,
        jnp.sum(own * own, axis=0, keepdims=True),
        jnp.where(row8 == 1, small_rows[1:2, :rows], jnp.where(row8 == 2, padded_tail, 0.0)),
    )
    pl.semaphore_wait(barrier, len(greet))

    def remote(src, dst, send, recv, peer):
        return pltpu.make_async_remote_copy(
            src_ref=src, dst_ref=dst, send_sem=send, recv_sem=recv, device_id=peer, device_id_type=MESH
        )

    half = width // 2
    top, bottom = pl.ds(0, half), pl.ds(half, half)

    def head_to_z(j):
        return remote(head, head_z.at[j - 1], head_send.at[j - 1], head_recv.at[j - 1], {"hy": z_peers[j]})

    def head_to_plane(i):
        return remote(head_mid, head_plane.at[i - 1], head_send.at[2 + i], head_recv.at[2 + i], {"hx": plane[i]})

    def gather_z(j):
        return remote(slots.at[0], slots.at[j], gather_send.at[j], gather_recv.at[j], {"hy": z_peers[j]})

    def gather_x(j):
        return remote(slots.at[j], slots.at[4 + j], gather_send.at[4 + j], gather_recv.at[4 + j], {"hx": along_x})

    def gather_y(j):
        return remote(slots.at[j], slots.at[8 + j], gather_send.at[8 + j], gather_recv.at[8 + j], {"hx": along_y})

    def relay_a(j):
        return remote(
            slots.at[4 + j, top], slots.at[12 + j, top], gather_send.at[12 + j], gather_recv.at[12 + j], {"hx": along_y}
        )

    def relay_b(j):
        return remote(
            slots.at[8 + j, bottom], slots.at[12 + j, bottom], gather_send.at[16 + j], gather_recv.at[16 + j], {"hx": along_x}
        )

    for j in (3, 2, 1):
        head_to_z(j).start()
    gather_x(0).start()
    gather_y(0).start()
    for j in (1, 2, 3):
        gather_z(j).start()
    weight_remote = []
    if paired:
        weight_remote = [
            remote(src, dst, weight_send.at[k], weight_recv.at[k], {"tok": 1 - c})
            for k, (src, dst) in enumerate(targets)
        ]
        for copy in weight_remote:
            copy.start()

    def forward(j):
        gather_z(j).wait_recv()
        gather_x(j).start()
        gather_y(j).start()

    def relay(j):
        gather_x(j).wait_recv()
        relay_a(j).start()
        gather_y(j).wait_recv()
        relay_b(j).start()

    for j in (1, 2, 3):
        head_to_z(j).wait_recv()
    mains = [head[...]] + [head_z[j] for j in range(3)]
    total = mains[0] + mains[1] + mains[2] + mains[3]
    tails = jnp.zeros((1, rows), F32)
    for j in range(4):
        part = mains[j][2:3, :LANES]
        if j:
            part = pltpu.roll(tall_row(part), j * rest, 1)[0:1]
        tails = tails + jnp.concatenate([part, jnp.zeros((1, rows - LANES), F32)], axis=1)
    mid = jnp.where(row8 == 0, total[0:1], 0.0)
    for j in range(4):
        mid = jnp.where(row8 == 1 + j, mains[j][1:2], mid)
    head_mid[...] = jnp.where(row8 == 5, tails, mid)
    for i in (3, 1, 2):
        head_to_plane(i).start()
    forward(1)
    relay(0)
    for i in (1, 2, 3):
        head_to_plane(i).wait_recv()
    groups = [head_mid[...]] + [head_plane[i] for i in range(3)]
    first_sq = groups[0][0:1] + groups[1][0:1] + groups[2][0:1] + groups[3][0:1]
    first_scale = lax.rsqrt(first_sq / D + epsilon)
    gain_columns = tall(jnp.concatenate(groups, axis=0))
    small_columns = tall(small_rows)
    for copy in weight_local[:3]:
        copy.wait()
    for copy in weight_remote[:3]:
        copy.wait_recv()

    def project(i, j):
        gain = jnp.concatenate(
            [gain_columns[:, 8 * i + 1 + j:8 * i + 2 + j], gain_columns[j * rest:(j + 1) * rest, 8 * i + 5:8 * i + 6]],
            axis=0,
        )
        normed = (slots[4 * i + j].astype(F32) * first_scale * gain).astype(BF16)
        part = lax.dot_general(
            weights[pl.ds(offset_of(i, j), width), :], normed, (((0,), (0,)), ((), ())), preferred_element_type=F32
        )
        if i == 0 and j == 0:
            acc[...] = part
        else:
            acc[...] += part

    shards, depth, columns = out_weight.shape

    def turn(k):
        span = 3 * LANES
        s, at = (k * span) // columns, (k * span) % columns
        out_t[k * span:(k + 1) * span, :] = out_weight[s, :, at:at + span].T

    def diagonal(j):
        relay_a(j).wait_recv()
        relay_b(j).wait_recv()
        project(3, j)

    project(0, 0)
    project(0, 1)
    forward(2)
    relay(1)
    project(0, 2)
    project(1, 0)
    project(2, 0)
    forward(3)
    relay(2)
    project(0, 3)
    project(1, 1)
    project(2, 1)
    diagonal(0)
    weight_local[3].wait()
    for copy in weight_remote[3:]:
        copy.wait_recv()
    turns = D // (3 * LANES)
    for k in range(turns // 2):
        turn(k)
    relay(3)
    project(1, 2)
    project(2, 2)
    diagonal(1)
    for k in range(turns // 2, turns):
        turn(k)
    project(1, 3)
    project(2, 3)
    locals_[2].wait()
    doc_row, doc_col = small_rows[0:1, :rows], small_columns[:rows, 0:1]
    s_index = lax.broadcasted_iota(jnp.int32, (LENGTH, LENGTH), 0)
    t_index = lax.broadcasted_iota(jnp.int32, (LENGTH, LENGTH), 1)
    diagonal(2)
    diagonal(3)

    cosine, sine = tables_v[0], tables_v[1]

    def rope(x):
        upper, lower = x[:HEAD // 2], x[HEAD // 2:]
        return jnp.concatenate([upper * cosine - lower * sine, lower * cosine + upper * sine], axis=0)

    query_heads, key_heads = qcols // HEAD, kcols // HEAD
    ratio = query_heads // key_heads
    allowed = (s_index <= t_index) & (doc_row == doc_col)
    attended = []
    for h in range(query_heads):
        kv = h // ratio
        query = (rope(acc[h * HEAD:(h + 1) * HEAD]) * (D / QH) ** (-0.5)).astype(BF16)
        key = rope(acc[qcols + kv * HEAD:qcols + (kv + 1) * HEAD]).astype(BF16)
        value = acc[qcols + kcols + kv * HEAD:qcols + kcols + (kv + 1) * HEAD].astype(BF16)
        scores = lax.dot_general(key, query, (((0,), (0,)), ((), ())), preferred_element_type=F32)
        best = jnp.max(jnp.where(allowed, scores, neg_big), axis=0, keepdims=True)
        soft = jnp.where(allowed, jnp.exp(scores - best), 0.0)
        mass = jnp.sum(soft, axis=0, keepdims=True)
        blended = jnp.dot(value, soft.astype(BF16), preferred_element_type=F32)
        attended.append((blended / mass).astype(BF16))
    attended = jnp.concatenate(attended, axis=0)

    def term(i, j):
        at = offset_of(i, j)
        terms[4 * i + j] = jnp.dot(out_t[pl.ds(at, width), :], attended, preferred_element_type=F32).astype(BF16)

    def diagonal_a(j):
        return remote(terms.at[12 + j, top], first_a.at[j], reduce_send.at[j], reduce_recv.at[j], {"hx": along_x})

    def diagonal_b(j):
        return remote(
            terms.at[12 + j, bottom], first_b.at[j], reduce_send.at[4 + j], reduce_recv.at[4 + j], {"hx": along_y}
        )

    def reduce_x(j):
        return remote(terms.at[4 + j], from_x.at[j], reduce_send.at[8 + j], reduce_recv.at[8 + j], {"hx": along_x})

    def reduce_y(j):
        return remote(terms.at[8 + j], from_y.at[j], reduce_send.at[12 + j], reduce_recv.at[12 + j], {"hx": along_y})

    def reduce_z(j):
        return remote(
            terms.at[j], from_z.at[j - 1], reduce_send.at[15 + j], reduce_recv.at[15 + j], {"hy": z_peers[j]}
        )

    def first(j):
        term(3, j)
        diagonal_a(j).start()
        diagonal_b(j).start()

    def second(j):
        term(2, j)
        term(1, j)
        diagonal_a(j).wait_recv()
        terms[8 + j, top, :] = (terms[8 + j, top, :].astype(F32) + first_a[j].astype(F32)).astype(BF16)
        reduce_y(j).start()
        diagonal_b(j).wait_recv()
        terms[4 + j, bottom, :] = (terms[4 + j, bottom, :].astype(F32) + first_b[j].astype(F32)).astype(BF16)
        reduce_x(j).start()

    def plane_sum(j):
        reduce_x(j).wait_recv()
        reduce_y(j).wait_recv()
        return terms[j].astype(F32) + from_x[j].astype(F32) + from_y[j].astype(F32)

    def third(j):
        terms[j] = plane_sum(j).astype(BF16)
        reduce_z(j).start()

    first(3)
    first(2)
    for j in (3, 2, 1, 0):
        term(0, j)
    second(3)
    first(1)
    second(2)
    first(0)
    second(1)
    third(3)
    second(0)
    third(2)
    third(1)
    mixed = plane_sum(0)
    for j in (3, 2, 1):
        reduce_z(j).wait_recv()
        mixed = mixed + from_z[j - 1].astype(F32)

    wide = slots[0].astype(F32)
    after, feed_gain = small_columns[:width, 2:3], small_columns[:width, 3:4]
    branch = mixed * after
    stats[...] = jnp.where(
        row8 == 0,
        jnp.sum(mixed * mixed, axis=0, keepdims=True),
        jnp.where(
            row8 == 1,
            jnp.sum(wide * branch, axis=0, keepdims=True),
            jnp.sum(branch * branch, axis=0, keepdims=True),
        ),
    )

    def stat_plane(i):
        return remote(stats, stats_in.at[i - 1], stat_send.at[i - 1], stat_recv.at[i - 1], {"hx": plane[i]})

    def stat_z(j):
        return remote(stats_mid, stats_zin.at[j - 1], stat_send.at[2 + j], stat_recv.at[2 + j], {"hy": z_peers[j]})

    for i in (3, 2, 1):
        stat_plane(i).start()
    for i in (1, 2, 3):
        stat_plane(i).wait_recv()
    stats_mid[...] = stats[...] + stats_in[0] + stats_in[1] + stats_in[2]
    for j in (3, 2, 1):
        stat_z(j).start()
    for j in (1, 2, 3):
        stat_z(j).wait_recv()
    summed = stats_mid[...] + stats_zin[0] + stats_zin[1] + stats_zin[2]
    after_scale = lax.rsqrt(summed[0:1] / D + epsilon)
    feed_sq = first_sq + 2.0 * after_scale * summed[1:2] + after_scale * after_scale * summed[2:3]
    feed_scale = lax.rsqrt(feed_sq / D + epsilon)
    residual = (wide + mixed * after_scale * after).astype(BF16)
    residual_out[...] = residual
    feed_out[...] = (residual.astype(F32) * feed_scale * feed_gain).astype(BF16)

    for j in range(4):
        gather_x(j).wait_send()
        gather_y(j).wait_send()
        relay_a(j).wait_send()
        relay_b(j).wait_send()
        diagonal_a(j).wait_send()
        diagonal_b(j).wait_send()
        reduce_x(j).wait_send()
        reduce_y(j).wait_send()
    for j in (1, 2, 3):
        head_to_z(j).wait_send()
        head_to_plane(j).wait_send()
        gather_z(j).wait_send()
        reduce_z(j).wait_send()
        stat_plane(j).wait_send()
        stat_z(j).wait_send()
    for copy in weight_remote:
        copy.wait_send()


def per_device(paired, stream_in, before_gain, after_gain, feed_gain, query_weight, key_weight, value_weight, output_weight, documents):
    rows, width = stream_in.shape
    if not paired:
        query_weight, key_weight, value_weight = (
            lax.all_gather(piece, "tok", axis=0, tiled=True) for piece in (query_weight, key_weight, value_weight)
        )
        output_weight = lax.all_gather(output_weight, "tok", axis=1, tiled=True)
    span = rows + LANES
    which = lax.broadcasted_iota(jnp.int32, (8, span), 0)

    def wide_row(vector):
        return jnp.pad(vector.astype(F32), (0, span - vector.shape[0]))[None]

    small = jnp.where(
        which == 0,
        wide_row(documents),
        jnp.where(
            which == 1, wide_row(before_gain), jnp.where(which == 2, wide_row(after_gain), wide_row(feed_gain))
        ),
    )
    tables = jnp.asarray(rope_tables())
    qcols, kcols = query_weight.shape[1], key_weight.shape[1]
    shards = 2 if paired else 1
    depth = output_weight.shape[0]
    any_spec = pl.BlockSpec(memory_space=pl.ANY)
    vmem = pl.BlockSpec(memory_space=pltpu.VMEM)
    dma = pltpu.SemaphoreType.DMA
    block = (width, rows)
    residual, feed_input = pl.pallas_call(
        functools.partial(kernel, paired),
        out_shape=[jax.ShapeDtypeStruct(block, BF16)] * 2,
        in_specs=[any_spec] * 7,
        out_specs=[vmem] * 2,
        scratch_shapes=[
            pltpu.VMEM((16,) + block, BF16),
            pltpu.VMEM((8, span), F32),
            pltpu.VMEM((2, HEAD // 2, LENGTH), F32),
            pltpu.VMEM((D, qcols + 2 * kcols), BF16),
            pltpu.VMEM((shards, depth, output_weight.shape[1]), BF16),
            pltpu.VMEM((D, depth), BF16),
            pltpu.VMEM((qcols + 2 * kcols, rows), F32),
            pltpu.VMEM((16,) + block, BF16),
            pltpu.VMEM((4, width // 2, rows), BF16),
            pltpu.VMEM((4, width // 2, rows), BF16),
            pltpu.VMEM((4,) + block, BF16),
            pltpu.VMEM((4,) + block, BF16),
            pltpu.VMEM((3,) + block, BF16),
        ]
        + [pltpu.VMEM((8, rows), F32), pltpu.VMEM((3, 8, rows), F32)] * 4
        + [
            dma((7,)),
            dma((4,)),
            dma((4,)),
            dma((20,)),
            dma((20,)),
            dma((19,)),
            dma((19,)),
            dma((6,)),
            dma((6,)),
            dma((6,)),
            dma((6,)),
        ],
        compiler_params=pltpu.CompilerParams(
            collective_id=0, has_side_effects=True, vmem_limit_bytes=56 * 1024 * 1024
        ),
    )(stream_in.T, small, tables, query_weight, key_weight, value_weight, output_weight)
    return residual.T, feed_input.T


def solution(mesh):
    both = ("hx", "hy")
    in_specs = (
        P("tok", both),
        P(both),
        P(both),
        P(both),
        P("tok", both),
        P("tok", both),
        P("tok", both),
        P(both, "tok"),
        P("tok"),
    )
    out_specs = (P("tok", both), P("tok", both))
    paired = mesh.shape["tok"] == 2
    return jax.shard_map(
        functools.partial(per_device, paired), mesh=mesh, in_specs=in_specs, out_specs=out_specs, check_vma=False
    )
```

```python
import functools

import jax
import jax.numpy as jnp
import numpy as np
from jax import lax
from jax.experimental import pallas as pl
from jax.experimental.pallas import tpu as pltpu
from jax.sharding import PartitionSpec as P

D = 4608
QH = 32
HEAD = 128
LENGTH = 256
LANES = 128

epsilon = 1e-06
neg_big = -1e30
MESH = pl.DeviceIdType.MESH
F32 = jnp.float32
BF16 = jnp.bfloat16


def flip(index, mask):
    low = (index % 2 + mask % 2) % 2
    high = (index // 2 + mask // 2) % 2
    return low + 2 * high


def rope_tables():
    half = HEAD // 2
    frequency = (10000.0 ** (-np.arange(half, dtype=np.float32) / half)).astype(np.float32)
    angles = frequency[:, None] * np.arange(LENGTH, dtype=np.float32)[None, :]
    return np.stack([np.cos(angles), np.sin(angles)]).astype(np.float32)


def tall_row(row):
    return jnp.broadcast_to(row, (8, row.shape[1]))


def tall(block):
    return jnp.concatenate([block] * (LANES // block.shape[0]), axis=0).T


def kernel(
    paired,
    stream, docs, before, after_in, tables, wq, wk, wv, wo,
    branch_out, scale_out,
    slots, docs_v, before_v, after_v, tables_v, weights, out_weight, out_t, acc,
    terms, first_a, first_b, from_x, from_y, from_z,
    head, head_z, head_mid, head_plane, stats, stats_in, stats_mid, stats_zin,
    local_sem, weight_send, weight_recv, gather_send, gather_recv, reduce_send, reduce_recv,
    head_send, head_recv, stat_send, stat_recv,
):
    width, rows = stream.shape
    rest = width - rows
    a, b, c = lax.axis_index("hx"), lax.axis_index("hy"), lax.axis_index("tok")
    along_x, along_y, across = flip(a, 1), flip(a, 2), flip(a, 3)
    plane = (None, along_x, along_y, across)
    z_peers = [None] + [flip(b, j) for j in (1, 2, 3)]

    def offset_of(i, j):
        return pl.multiple_of((flip(a, i) * 4 + flip(b, j)) * width, 16)

    locals_ = [
        pltpu.make_async_copy(stream, slots.at[0], local_sem.at[0]),
        pltpu.make_async_copy(before, before_v, local_sem.at[1]),
        pltpu.make_async_copy(tables, tables_v, local_sem.at[2]),
        pltpu.make_async_copy(docs, docs_v, local_sem.at[7]),
        pltpu.make_async_copy(after_in, after_v, local_sem.at[8]),
    ]
    for copy in locals_:
        copy.start()
    wrows, qcols, kcols = wq.shape[0], wq.shape[1], wk.shape[1]
    shard = c if paired else 0
    start = pl.multiple_of(shard * wrows, 16)
    targets = [
        (wq, weights.at[pl.ds(start, wrows), pl.ds(0, qcols)]),
        (wk, weights.at[pl.ds(start, wrows), pl.ds(qcols, kcols)]),
        (wv, weights.at[pl.ds(start, wrows), pl.ds(qcols + kcols, kcols)]),
        (wo, out_weight.at[shard]),
    ]
    weight_local = [
        pltpu.make_async_copy(src, dst, local_sem.at[3 + k]) for k, (src, dst) in enumerate(targets)
    ]

    barrier = pltpu.get_barrier_semaphore()
    greet = [{"hx": along_x}, {"hx": along_y}, {"hx": across}]
    greet += [{"hy": z_peers[j]} for j in (1, 2, 3)]
    if paired:
        greet.append({"tok": 1 - c})
    for peer in greet:
        pl.semaphore_signal(barrier, inc=1, device_id=peer, device_id_type=MESH)
    for copy in weight_local:
        copy.start()

    row8 = lax.broadcasted_iota(jnp.int32, (8, rows), 0)
    locals_[0].wait()
    locals_[1].wait()
    own = slots[0].astype(F32)
    def padded(vector):
        wide_vector = vector.astype(F32)
        return jnp.concatenate([wide_vector, jnp.zeros((1, rows + LANES - vector.shape[1]), F32)], axis=1)

    before_row = padded(before_v[...])
    padded_tail = jnp.concatenate([before_row[:, rows:], jnp.zeros((1, rows - LANES), F32)], axis=1)
    head[...] = jnp.where(
        row8 == 0,
        jnp.sum(own * own, axis=0, keepdims=True),
        jnp.where(row8 == 1, before_row[:, :rows], jnp.where(row8 == 2, padded_tail, 0.0)),
    )
    pl.semaphore_wait(barrier, len(greet))

    def remote(src, dst, send, recv, peer):
        return pltpu.make_async_remote_copy(
            src_ref=src, dst_ref=dst, send_sem=send, recv_sem=recv, device_id=peer, device_id_type=MESH
        )

    half = width // 2
    top, bottom = pl.ds(0, half), pl.ds(half, half)

    def head_to_z(j):
        return remote(head, head_z.at[j - 1], head_send.at[j - 1], head_recv.at[j - 1], {"hy": z_peers[j]})

    def head_to_plane(i):
        return remote(head_mid, head_plane.at[i - 1], head_send.at[2 + i], head_recv.at[2 + i], {"hx": plane[i]})

    halves = (top, bottom)

    def gather_z(j):
        return remote(slots.at[0], slots.at[j], gather_send.at[j], gather_recv.at[j], {"hy": z_peers[j]})

    def gather_z3(h):
        part = halves[h]
        return remote(
            slots.at[0, part], slots.at[3, part], gather_send.at[20 + h], gather_recv.at[20 + h], {"hy": z_peers[3]}
        )

    def gather_x3(h):
        part = halves[h]
        return remote(
            slots.at[3, part], slots.at[7, part], gather_send.at[22 + h], gather_recv.at[22 + h], {"hx": along_x}
        )

    def gather_y3(h):
        part = halves[h]
        return remote(
            slots.at[3, part], slots.at[11, part], gather_send.at[24 + h], gather_recv.at[24 + h], {"hx": along_y}
        )

    def across_z(j, h):
        part, k = halves[h], (13 if j == 0 else 26) + h * 2
        return remote(
            slots.at[12 + j, part], slots.at[13 + j, part], gather_send.at[k], gather_recv.at[k], {"hy": z_peers[1]}
        )

    def gather_x(j):
        return remote(slots.at[j], slots.at[4 + j], gather_send.at[4 + j], gather_recv.at[4 + j], {"hx": along_x})

    def gather_y(j):
        return remote(slots.at[j], slots.at[8 + j], gather_send.at[8 + j], gather_recv.at[8 + j], {"hx": along_y})

    def relay_a(j):
        return remote(
            slots.at[4 + j, top], slots.at[12 + j, top], gather_send.at[12 + j], gather_recv.at[12 + j], {"hx": along_y}
        )

    def relay_b(j):
        return remote(
            slots.at[8 + j, bottom], slots.at[12 + j, bottom], gather_send.at[16 + j], gather_recv.at[16 + j], {"hx": along_x}
        )

    for j in (3, 2, 1):
        head_to_z(j).start()
    gather_x(0).start()
    gather_y(0).start()
    for j in (1, 2):
        gather_z(j).start()
    gather_z3(0).start()
    gather_z3(1).start()
    weight_remote = []
    if paired:
        weight_remote = [
            remote(src, dst, weight_send.at[k], weight_recv.at[k], {"tok": 1 - c})
            for k, (src, dst) in enumerate(targets)
        ]
        for copy in weight_remote:
            copy.start()

    def forward(j):
        gather_z(j).wait_recv()
        gather_x(j).start()
        gather_y(j).start()

    def relay(j):
        gather_x(j).wait_recv()
        relay_a(j).start()
        gather_y(j).wait_recv()
        relay_b(j).start()

    def spread(j):
        relay_a(j).wait_recv()
        across_z(j, 0).start()
        relay_b(j).wait_recv()
        across_z(j, 1).start()

    for j in (1, 2, 3):
        head_to_z(j).wait_recv()
    mains = [head[...]] + [head_z[j] for j in range(3)]
    total = mains[0] + mains[1] + mains[2] + mains[3]
    tails = jnp.zeros((1, rows), F32)
    for j in range(4):
        part = mains[j][2:3, :LANES]
        if j:
            part = pltpu.roll(tall_row(part), j * rest, 1)[0:1]
        tails = tails + jnp.concatenate([part, jnp.zeros((1, rows - LANES), F32)], axis=1)
    mid = jnp.where(row8 == 0, total[0:1], 0.0)
    for j in range(4):
        mid = jnp.where(row8 == 1 + j, mains[j][1:2], mid)
    head_mid[...] = jnp.where(row8 == 5, tails, mid)
    for i in (3, 1, 2):
        head_to_plane(i).start()
    forward(1)
    relay(0)
    for i in (1, 2, 3):
        head_to_plane(i).wait_recv()
    groups = [head_mid[...]] + [head_plane[i] for i in range(3)]
    first_sq = groups[0][0:1] + groups[1][0:1] + groups[2][0:1] + groups[3][0:1]
    first_scale = lax.rsqrt(first_sq / D + epsilon)
    gain_columns = tall(jnp.concatenate(groups, axis=0))
    for copy in weight_local[:3]:
        copy.wait()
    for copy in weight_remote[:3]:
        copy.wait_recv()

    def project(i, j):
        gain = jnp.concatenate(
            [gain_columns[:, 8 * i + 1 + j:8 * i + 2 + j], gain_columns[j * rest:(j + 1) * rest, 8 * i + 5:8 * i + 6]],
            axis=0,
        )
        normed = (slots[4 * i + j].astype(F32) * first_scale * gain).astype(BF16)
        part = lax.dot_general(
            weights[pl.ds(offset_of(i, j), width), :], normed, (((0,), (0,)), ((), ())), preferred_element_type=F32
        )
        if i == 0 and j == 0:
            acc[...] = part
        else:
            acc[...] += part

    shards, depth, columns = out_weight.shape

    def turn(k):
        span = 3 * LANES
        s, at = (k * span) // columns, (k * span) % columns
        out_t[k * span:(k + 1) * span, :] = out_weight[s, :, at:at + span].T

    project(0, 0)
    project(0, 1)
    forward(2)
    spread(0)
    project(0, 2)
    gather_x(1).wait_recv()
    gather_y(1).wait_recv()
    project(1, 0)
    project(2, 0)
    relay(2)
    for h in range(2):
        gather_z3(h).wait_recv()
        gather_x3(h).start()
        gather_y3(h).start()
    project(0, 3)
    project(1, 1)
    project(2, 1)
    project(3, 0)
    spread(2)
    weight_local[3].wait()
    for copy in weight_remote[3:]:
        copy.wait_recv()
    turns = D // (3 * LANES)
    for k in range(turns):
        turn(k)
    project(1, 2)
    project(2, 2)
    across_z(0, 0).wait_recv()
    across_z(0, 1).wait_recv()
    project(3, 1)
    project(3, 2)
    locals_[2].wait()
    locals_[3].wait()
    locals_[4].wait()
    doc_row = docs_v[...].astype(F32)
    after_row = padded(after_v[...])
    doc_col = tall(jnp.broadcast_to(doc_row, (8, rows)))[:, 0:1]
    after = tall(jnp.broadcast_to(after_row, (8, rows + LANES)))[:width, 0:1]
    s_index = lax.broadcasted_iota(jnp.int32, (LENGTH, LENGTH), 0)
    t_index = lax.broadcasted_iota(jnp.int32, (LENGTH, LENGTH), 1)
    for h in range(2):
        gather_x3(h).wait_recv()
        gather_y3(h).wait_recv()
    project(1, 3)
    project(2, 3)
    across_z(2, 0).wait_recv()
    across_z(2, 1).wait_recv()
    project(3, 3)

    cosine, sine = tables_v[0], tables_v[1]

    def rope(x):
        upper, lower = x[:HEAD // 2], x[HEAD // 2:]
        return jnp.concatenate([upper * cosine - lower * sine, lower * cosine + upper * sine], axis=0)

    query_heads, key_heads = qcols // HEAD, kcols // HEAD
    ratio = query_heads // key_heads
    allowed = (s_index <= t_index) & (doc_row == doc_col)
    attended = []
    for h in range(query_heads):
        kv = h // ratio
        query = (rope(acc[h * HEAD:(h + 1) * HEAD]) * (D / QH) ** (-0.5)).astype(BF16)
        key = rope(acc[qcols + kv * HEAD:qcols + (kv + 1) * HEAD]).astype(BF16)
        value = acc[qcols + kcols + kv * HEAD:qcols + kcols + (kv + 1) * HEAD].astype(BF16)
        scores = lax.dot_general(key, query, (((0,), (0,)), ((), ())), preferred_element_type=F32)
        best = jnp.max(jnp.where(allowed, scores, neg_big), axis=0, keepdims=True)
        soft = jnp.where(allowed, jnp.exp(scores - best), 0.0)
        mass = jnp.sum(soft, axis=0, keepdims=True)
        blended = jnp.dot(value, soft.astype(BF16), preferred_element_type=F32)
        attended.append((blended / mass).astype(BF16))
    attended = jnp.concatenate(attended, axis=0)

    def term(i, j):
        at = offset_of(i, j)
        terms[4 * i + j] = jnp.dot(out_t[pl.ds(at, width), :], attended, preferred_element_type=F32).astype(BF16)

    def diagonal_a(j):
        return remote(terms.at[12 + j, top], first_a.at[j], reduce_send.at[j], reduce_recv.at[j], {"hx": along_x})

    def diagonal_b(j):
        return remote(
            terms.at[12 + j, bottom], first_b.at[j], reduce_send.at[4 + j], reduce_recv.at[4 + j], {"hx": along_y}
        )

    def reduce_x(j):
        return remote(terms.at[4 + j], from_x.at[j], reduce_send.at[8 + j], reduce_recv.at[8 + j], {"hx": along_x})

    def reduce_y(j):
        return remote(terms.at[8 + j], from_y.at[j], reduce_send.at[12 + j], reduce_recv.at[12 + j], {"hx": along_y})

    def reduce_z(j):
        return remote(
            terms.at[j], from_z.at[j - 1], reduce_send.at[15 + j], reduce_recv.at[15 + j], {"hy": z_peers[j]}
        )

    def last_x(h):
        part = halves[h]
        return remote(
            terms.at[5, part], from_x.at[1, part], reduce_send.at[19 + h], reduce_recv.at[19 + h], {"hx": along_x}
        )

    def last_y(h):
        part = halves[h]
        return remote(
            terms.at[9, part], from_y.at[1, part], reduce_send.at[21 + h], reduce_recv.at[21 + h], {"hx": along_y}
        )

    def last_z(h):
        part = halves[h]
        return remote(
            terms.at[1, part], from_z.at[0, part], reduce_send.at[23 + h], reduce_recv.at[23 + h], {"hy": z_peers[1]}
        )

    def first(j):
        term(3, j)
        diagonal_a(j).start()
        diagonal_b(j).start()

    def second(j):
        term(2, j)
        term(1, j)
        diagonal_a(j).wait_recv()
        terms[8 + j, top, :] = (terms[8 + j, top, :].astype(F32) + first_a[j].astype(F32)).astype(BF16)
        if j == 1:
            last_y(0).start()
            last_y(1).start()
        else:
            reduce_y(j).start()
        diagonal_b(j).wait_recv()
        terms[4 + j, bottom, :] = (terms[4 + j, bottom, :].astype(F32) + first_b[j].astype(F32)).astype(BF16)
        if j == 1:
            last_x(0).start()
            last_x(1).start()
        else:
            reduce_x(j).start()

    def plane_sum(j):
        reduce_x(j).wait_recv()
        reduce_y(j).wait_recv()
        return terms[j].astype(F32) + from_x[j].astype(F32) + from_y[j].astype(F32)

    def third(j):
        terms[j] = plane_sum(j).astype(BF16)
        reduce_z(j).start()

    first(3)
    first(2)
    for j in (3, 2, 1, 0):
        term(0, j)
    second(3)
    first(1)
    second(2)
    first(0)
    second(1)
    third(3)
    second(0)
    third(2)
    for h in range(2):
        last_x(h).wait_recv()
        last_y(h).wait_recv()
        part = halves[h]
        summed = terms[1, part, :].astype(F32) + from_x[1, part, :].astype(F32) + from_y[1, part, :].astype(F32)
        terms[1, part, :] = summed.astype(BF16)
        last_z(h).start()
    mixed = plane_sum(0)
    for j in (3, 2, 1):
        if j == 1:
            last_z(0).wait_recv()
            last_z(1).wait_recv()
        else:
            reduce_z(j).wait_recv()
        mixed = mixed + from_z[j - 1].astype(F32)

    wide = slots[0].astype(F32)
    branch = mixed * after
    stats[...] = jnp.where(
        row8 == 0,
        jnp.sum(mixed * mixed, axis=0, keepdims=True),
        jnp.where(
            row8 == 1,
            jnp.sum(wide * branch, axis=0, keepdims=True),
            jnp.sum(branch * branch, axis=0, keepdims=True),
        ),
    )

    def stat_plane(i):
        return remote(stats, stats_in.at[i - 1], stat_send.at[i - 1], stat_recv.at[i - 1], {"hx": plane[i]})

    def stat_z(j):
        return remote(stats_mid, stats_zin.at[j - 1], stat_send.at[2 + j], stat_recv.at[2 + j], {"hy": z_peers[j]})

    for i in (3, 2, 1):
        stat_plane(i).start()
    for i in (1, 2, 3):
        stat_plane(i).wait_recv()
    stats_mid[...] = stats[...] + stats_in[0] + stats_in[1] + stats_in[2]
    for j in (3, 2, 1):
        stat_z(j).start()
    for j in (1, 2, 3):
        stat_z(j).wait_recv()
    summed = stats_mid[...] + stats_zin[0] + stats_zin[1] + stats_zin[2]
    after_scale = lax.rsqrt(summed[0:1] / D + epsilon)
    feed_sq = first_sq + 2.0 * after_scale * summed[1:2] + after_scale * after_scale * summed[2:3]
    feed_scale = lax.rsqrt(feed_sq / D + epsilon)
    branch_out[...] = branch
    scale_out[...] = jnp.where(row8 == 0, after_scale, feed_scale)

    for j in range(4):
        if j < 3:
            gather_x(j).wait_send()
            gather_y(j).wait_send()
        diagonal_a(j).wait_send()
        diagonal_b(j).wait_send()
        if j != 1:
            reduce_x(j).wait_send()
            reduce_y(j).wait_send()
    for j in (0, 2):
        relay_a(j).wait_send()
        relay_b(j).wait_send()
    for h in range(2):
        for copy in (gather_z3, gather_x3, gather_y3, last_x, last_y, last_z):
            copy(h).wait_send()
        across_z(0, h).wait_send()
        across_z(2, h).wait_send()
    for j in (1, 2, 3):
        head_to_z(j).wait_send()
        head_to_plane(j).wait_send()
        stat_plane(j).wait_send()
        stat_z(j).wait_send()
    for j in (1, 2):
        gather_z(j).wait_send()
    for j in (2, 3):
        reduce_z(j).wait_send()
    for copy in weight_remote:
        copy.wait_send()


def per_device(paired, stream_in, before_gain, after_gain, feed_gain, query_weight, key_weight, value_weight, output_weight, documents):
    rows, width = stream_in.shape
    if not paired:
        query_weight, key_weight, value_weight = (
            lax.all_gather(piece, "tok", axis=0, tiled=True) for piece in (query_weight, key_weight, value_weight)
        )
        output_weight = lax.all_gather(output_weight, "tok", axis=1, tiled=True)
    tables = jnp.asarray(rope_tables())
    qcols, kcols = query_weight.shape[1], key_weight.shape[1]
    shards = 2 if paired else 1
    depth = output_weight.shape[0]
    any_spec = pl.BlockSpec(memory_space=pl.ANY)
    vmem = pl.BlockSpec(memory_space=pltpu.VMEM)
    dma = pltpu.SemaphoreType.DMA
    block = (width, rows)
    branch, scales = pl.pallas_call(
        functools.partial(kernel, paired),
        out_shape=[jax.ShapeDtypeStruct(block, F32), jax.ShapeDtypeStruct((8, rows), F32)],
        in_specs=[any_spec] * 9,
        out_specs=[vmem] * 2,
        scratch_shapes=[
            pltpu.VMEM((16,) + block, BF16),
            pltpu.VMEM((1, rows), jnp.int32),
            pltpu.VMEM((1, width), BF16),
            pltpu.VMEM((1, width), BF16),
            pltpu.VMEM((2, HEAD // 2, LENGTH), F32),
            pltpu.VMEM((D, qcols + 2 * kcols), BF16),
            pltpu.VMEM((shards, depth, output_weight.shape[1]), BF16),
            pltpu.VMEM((D, depth), BF16),
            pltpu.VMEM((qcols + 2 * kcols, rows), F32),
            pltpu.VMEM((16,) + block, BF16),
            pltpu.VMEM((4, width // 2, rows), BF16),
            pltpu.VMEM((4, width // 2, rows), BF16),
            pltpu.VMEM((4,) + block, BF16),
            pltpu.VMEM((4,) + block, BF16),
            pltpu.VMEM((3,) + block, BF16),
        ]
        + [pltpu.VMEM((8, rows), F32), pltpu.VMEM((3, 8, rows), F32)] * 4
        + [
            dma((9,)),
            dma((4,)),
            dma((4,)),
            dma((29,)),
            dma((29,)),
            dma((25,)),
            dma((25,)),
            dma((6,)),
            dma((6,)),
            dma((6,)),
            dma((6,)),
        ],
        compiler_params=pltpu.CompilerParams(
            collective_id=0, has_side_effects=True, vmem_limit_bytes=56 * 1024 * 1024
        ),
    )(
        stream_in.T,
        documents.reshape(1, rows),
        before_gain.reshape(1, width),
        after_gain.reshape(1, width),
        tables,
        query_weight,
        key_weight,
        value_weight,
        output_weight,
    )
    after_scale, feed_scale = scales[0][:, None], scales[1][:, None]
    wide = stream_in.astype(F32)
    residual = (wide + branch.T * after_scale).astype(BF16)
    feed_input = (residual.astype(F32) * feed_scale * feed_gain.astype(F32)[None, :]).astype(BF16)
    return residual, feed_input


def solution(mesh):
    both = ("hx", "hy")
    in_specs = (
        P("tok", both),
        P(both),
        P(both),
        P(both),
        P("tok", both),
        P("tok", both),
        P("tok", both),
        P(both, "tok"),
        P("tok"),
    )
    out_specs = (P("tok", both), P("tok", both))
    paired = mesh.shape["tok"] == 2
    return jax.shard_map(
        functools.partial(per_device, paired), mesh=mesh, in_specs=in_specs, out_specs=out_specs, check_vma=False
    )
```
